1024 devices in a mesh: lat: 32 (over x, y, core), lon: 32 (over z).
Axes of the slice: x: 4, y: 4, z: 32, core: 2. Of those that a mesh axis runs over, the one named last changes fastest.
Arguments:
- prediction_deviation: bfloat16 [16, 1024, 1024, 80], P(None, 'lat', 'lon'), may hold values from -6 to 6
- humid_energy_misfit: float32 [16, 1024, 1024], P(None, 'lat', 'lon'), may hold values from -0.6 to 0.6
- sensor_space_deviation: bfloat16 [32, 32, 80, 1024], P('lat', 'lon'), may hold values from -6 to 6
- scaled_departure: float32 [32, 32, 1024], P('lat', 'lon'), may hold values from -6 to 6
- datum_location: int32 [32, 32, 2, 1024], P('lat', 'lon'), may hold values from 0 to 31, as said below
- taper_category: int32 [32, 32, 1024], P('lat', 'lon'), may hold values from 0 to 3
- datum_patch_codes: int32 [32, 32, 4, 1024], P('lat', 'lon'), may hold values from -1 to 8, as said below
- active_datum_tally: int32 [32, 32], P('lat', 'lon'), may hold values from 128 to 1024, as said below
Outputs:
- impact: float32 [32, 32, 1024], P('lat', 'lon')
The draws below stay inside these ranges and needn't reach their ends.
Inputs may be any that keep to these rules, and one draw needn't show every extreme that they name: `datum_location`: row and column of the observation's cell, each from 0 to 31. `datum_patch_codes`: codes are 3 (dr + 1) + (ds + 1) for a tile offset (dr, ds) from the owner, or -1 for an empty entry. Entry 0 is always 4, the owner; the named codes of a slot are distinct and never name a tile beyond the first or last tile row. At least 128 live slots on every tile, and 1024 on some tile in every draw; slots from active_datum_tally on carry no observation.
All inputs are finite; a program needn't handle non-finite values.
Results may differ from the reference program's by a relative error of at most 0.0055.
Values may be sent and summed in bfloat16 or wider, within the bound.
No kernel may reach another device: no remote copies, remote signals or barrier semaphores. Data moves between devices by JAX's collectives and lax.ppermute only.
A program may use at most 32 MiB of HBM per device.

```python
import jax
import jax.numpy as jnp
from jax import lax

RUN_TOTAL = 80
STRATA_TOTAL = 16
TW = 32
OBS_DEV = 1024
LAT_TILES = 32
LON_TILES = 32
NORTH_SOUTH_SPAN = 1024
EAST_WEST_SPAN = 1024


def obs_geometry(key):
    base = jax.random.fold_in(key, 7)
    first, second, third = jax.random.split(base, 3)
    array_shape = (LAT_TILES, LON_TILES, OBS_DEV)
    rows_drawn = jax.random.randint(first, array_shape, 0, TW, dtype=jnp.int32)
    cols_drawn = jax.random.randint(second, array_shape, 0, TW, dtype=jnp.int32)
    classes = jax.random.randint(third, array_shape, 0, 4, dtype=jnp.int32)
    return (rows_drawn, cols_drawn, classes)


def draw_humid_energy_misfit(key, part):
    base = jax.random.fold_in(key, 23)
    first = jax.random.fold_in(base, 0)
    array_shape = (STRATA_TOTAL, NORTH_SOUTH_SPAN, EAST_WEST_SPAN)
    drawn = 0.1 * jnp.clip(jax.random.normal(first, array_shape, jnp.float32), -6.0, 6.0)
    return drawn.astype(jnp.float32)


def draw_scaled_departure(key, part):
    base = jax.random.fold_in(key, 29)
    first = jax.random.fold_in(base, 0)
    array_shape = (LAT_TILES, LON_TILES, OBS_DEV)
    drawn = jnp.clip(jax.random.normal(first, array_shape, jnp.float32), -6.0, 6.0)
    return drawn.astype(jnp.float32)


def draw_datum_location(key, part):
    rows_drawn, cols_drawn, classes = obs_geometry(key)
    return jnp.stack([rows_drawn, cols_drawn], axis=2).astype(jnp.int32)


def draw_taper_category(key, part):
    rows_drawn, cols_drawn, classes = obs_geometry(key)
    return classes


def draw_datum_patch_codes(key, part):
    rows_drawn, cols_drawn, classes = obs_geometry(key)
    skipping = jax.random.randint(jax.random.fold_in(key, 13), rows_drawn.shape, 0, 8, dtype=jnp.int32)
    reach_cells = TW * (1 + classes)
    tile_rows = jnp.arange(LAT_TILES, dtype=jnp.int32)[:, None, None]
    upward = (8 * (rows_drawn + 1) < reach_cells) & (tile_rows > 0)
    downward = (8 * (TW - rows_drawn) < reach_cells) & (tile_rows < LAT_TILES - 1)
    leftward = 8 * (cols_drawn + 1) < reach_cells
    rightward = 8 * (TW - cols_drawn) < reach_cells
    row_step = jnp.where(upward, -1, jnp.where(downward, 1, 0))
    col_step = jnp.where(leftward, -1, jnp.where(rightward, 1, 0))
    has_row = upward | downward
    has_col = leftward | rightward
    own_code = jnp.full(rows_drawn.shape, 4, jnp.int32)
    row_code = jnp.where(has_row & (skipping != 1), 3 * (row_step + 1) + 1, -1)
    col_code = jnp.where(has_col & (skipping != 2), 3 + col_step + 1, -1)
    corner_code = jnp.where(has_row & has_col & (skipping != 0), 3 * (row_step + 1) + col_step + 1, -1)
    return jnp.stack([own_code, row_code, col_code, corner_code], axis=2).astype(jnp.int32)


def draw_active_datum_tally(key, part):
    base = jax.random.fold_in(key, 11)
    first, second, third, fourth = jax.random.split(base, 4)
    array_shape = (LAT_TILES, LON_TILES)
    drawn = jax.random.randint(first, array_shape, OBS_DEV // 8, OBS_DEV // 2 + 1, dtype=jnp.int32)
    crowded = jax.random.randint(second, array_shape, 0, 4, dtype=jnp.int32) == 0
    dense = OBS_DEV - jax.random.randint(third, array_shape, 0, OBS_DEV // 8, dtype=jnp.int32)
    counts = jnp.where(crowded, dense, drawn)
    chosen = jax.random.randint(fourth, (), 0, LAT_TILES * LON_TILES, dtype=jnp.int32)
    flat_index = jnp.arange(LAT_TILES * LON_TILES, dtype=jnp.int32).reshape(array_shape)
    return jnp.where(flat_index == chosen, OBS_DEV, counts).astype(jnp.int32)


def steps_of(key, extent, cuts, smallest, top_value):
    factor_of, own = 1.0, jax.random.fold_in(key, 6)
    for dim, shards_of in cuts:
        draws = jnp.exp(jax.random.uniform(jax.random.fold_in(own, dim), (shards_of,), jnp.float32, smallest / len(cuts), top_value / len(cuts)))
        factor_of = factor_of * jnp.repeat(draws, extent[dim] // shards_of).reshape([-1 if axis == dim else 1 for axis in range(len(extent))])
    return factor_of


def noise(own_key, dims, spread, bound, pieces=(), kind=jnp.bfloat16):
    factor_of = steps_of(own_key, dims, pieces, -0.22, 0.18) if pieces else 1.0
    array = jax.random.normal(own_key, dims, jnp.float32) * spread * factor_of
    return jnp.minimum(jnp.maximum(array, -bound), bound).astype(kind)


def setup_inputs(seed: int = 0) -> dict:
    key_list = jax.random.split(jax.random.key(seed), 9)
    prediction_deviation = noise(key_list[0], (STRATA_TOTAL, NORTH_SOUTH_SPAN, EAST_WEST_SPAN, RUN_TOTAL), 1.0, 6.0, ((1, 32), (2, 32)))
    humid_energy_misfit = draw_humid_energy_misfit(jax.random.fold_in(key_list[8], 71), 0)
    sensor_space_deviation = noise(key_list[2], (LAT_TILES, LON_TILES, RUN_TOTAL, OBS_DEV), 1.0, 6.0, ((0, 32), (1, 32)))
    scaled_departure = draw_scaled_departure(jax.random.fold_in(key_list[8], 71), 0)
    datum_location = draw_datum_location(jax.random.fold_in(key_list[8], 71), 0)
    taper_category = draw_taper_category(jax.random.fold_in(key_list[8], 71), 0)
    datum_patch_codes = draw_datum_patch_codes(jax.random.fold_in(key_list[8], 71), 0)
    active_datum_tally = draw_active_datum_tally(jax.random.fold_in(key_list[8], 71), 0)
    return dict(prediction_deviation=prediction_deviation, humid_energy_misfit=humid_energy_misfit, sensor_space_deviation=sensor_space_deviation, scaled_departure=scaled_departure, datum_location=datum_location, taper_category=taper_category, datum_patch_codes=datum_patch_codes, active_datum_tally=active_datum_tally)


def taper_weights(obs_row, obs_col, obs_class, cell_rows, cell_cols, allowed, patch_span_points):
    radius = patch_span_points * (1.0 + obs_class) * 0.125
    radius_sq = (radius * radius)[:, None]
    distance = (cell_rows[None, :] - obs_row[:, None]) ** 2 + (cell_cols[None, :] - obs_col[:, None]) ** 2
    fraction = 1.0 - distance / radius_sq
    return jnp.where(allowed & (distance < radius_sq), fraction * fraction, 0.0).astype(jnp.bfloat16)


def tile_offset(shifted, patch_span_points):
    return (shifted >= patch_span_points).astype(jnp.int32) - (shifted < 0).astype(jnp.int32)


def reference(prediction_deviation, humid_energy_misfit, sensor_space_deviation, scaled_departure, datum_location, taper_category, datum_patch_codes, active_datum_tally):
    patch_span_points = TW
    margin = TW // 2
    window_width = 2 * TW

    def add_level(stratum_index, summed):
        altitude_stratum = lax.dynamic_index_in_dim(prediction_deviation, stratum_index, 0, keepdims=False).astype(jnp.float32)
        weight = lax.dynamic_index_in_dim(humid_energy_misfit, stratum_index, 0, keepdims=False)
        return summed + altitude_stratum * weight[..., None]

    summed = lax.fori_loop(0, STRATA_TOTAL, add_level, jnp.zeros((NORTH_SOUTH_SPAN, EAST_WEST_SPAN, RUN_TOTAL), jnp.float32))
    projected = summed.astype(jnp.bfloat16)
    padded = jnp.pad(projected, ((margin, margin), (0, 0), (0, 0)))
    padded = jnp.concatenate([padded[:, EAST_WEST_SPAN - margin:], padded, padded[:, :margin]], axis=1)

    offsets = jnp.arange(window_width, dtype=jnp.int32) - margin
    rel_rows = jnp.repeat(offsets, window_width)
    rel_cols = jnp.tile(offsets, window_width)
    tile_code = 3 * (tile_offset(rel_rows, patch_span_points) + 1) + tile_offset(rel_cols, patch_span_points) + 1
    cell_rows = rel_rows.astype(jnp.float32)
    cell_cols = rel_cols.astype(jnp.float32)

    tile_total = LAT_TILES * LON_TILES
    anomaly_all = sensor_space_deviation.reshape(tile_total, RUN_TOTAL, OBS_DEV)
    innovation_all = scaled_departure.reshape(tile_total, OBS_DEV)
    place_all = datum_location.reshape(tile_total, 2, OBS_DEV)
    class_all = taper_category.reshape(tile_total, OBS_DEV)
    cover_all = datum_patch_codes.reshape(tile_total, 4, OBS_DEV)
    count_all = active_datum_tally.reshape(tile_total)

    def one_tile(tile_index):
        tile_row = tile_index // LON_TILES
        tile_col = tile_index % LON_TILES
        window = lax.dynamic_slice(padded, (tile_row * patch_span_points, tile_col * patch_span_points, jnp.int32(0)),
                                   (window_width, window_width, RUN_TOTAL)).reshape(window_width * window_width, RUN_TOTAL)
        anomaly = lax.dynamic_index_in_dim(anomaly_all, tile_index, 0, keepdims=False)
        scaled = lax.dynamic_index_in_dim(innovation_all, tile_index, 0, keepdims=False)
        position = lax.dynamic_index_in_dim(place_all, tile_index, 0, keepdims=False).astype(jnp.float32)
        taper_size = lax.dynamic_index_in_dim(class_all, tile_index, 0, keepdims=False).astype(jnp.float32)
        cover_codes = lax.dynamic_index_in_dim(cover_all, tile_index, 0, keepdims=False)
        count_here = lax.dynamic_index_in_dim(count_all, tile_index, 0, keepdims=False)
        allowed = jnp.any(cover_codes[:, :, None] == tile_code[None, None, :], axis=0)
        weights = taper_weights(position[0], position[1], taper_size, cell_rows, cell_cols, allowed, patch_span_points)
        projection = jnp.dot(weights.astype(jnp.float32), window.astype(jnp.float32),
                             precision=lax.Precision.HIGHEST)
        summed_here = jnp.sum(projection * anomaly.T.astype(jnp.float32), axis=1)
        live_slots = (jnp.arange(OBS_DEV, dtype=jnp.int32) < count_here).astype(jnp.float32)
        return scaled * summed_here / (RUN_TOTAL - 1) * live_slots

    impacts = lax.map(one_tile, jnp.arange(tile_total, dtype=jnp.int32))
    return impacts.reshape(LAT_TILES, LON_TILES, OBS_DEV)
```

```python
import jax
import jax.numpy as jnp
from jax import lax
from jax.experimental import pallas as pl
from jax.experimental.pallas import tpu as pltpu
from jax.sharding import PartitionSpec as P

HALF = 16
CELLS = HALF * HALF
CHUNKS = 4

F32 = jnp.float32
BF16 = jnp.bfloat16


def level_sum_kernel(dev_hbm, misfit_hbm, left_ref, right_ref, dev, misfit_ref, wide, sems):
    levels, rows, cols, runs = dev.shape
    step = rows // CHUNKS
    first = pltpu.make_async_copy(misfit_hbm, misfit_ref, sems.at[CHUNKS])
    first.start()
    copies = []
    for c in range(CHUNKS):
        part = pl.ds(c * step, step)
        copies.append(pltpu.make_async_copy(dev_hbm.at[:, part], dev.at[:, part], sems.at[c]))
        copies[-1].start()
    first.wait()
    for h in range(cols // HALF):
        wide[h] = jnp.concatenate(
            [misfit_ref[l][:, h * HALF : (h + 1) * HALF] for l in range(levels)], axis=1
        )
    depth = levels * HALF
    own = lax.broadcasted_iota(jnp.int32, (HALF, depth), 0)
    lane = lax.broadcasted_iota(jnp.int32, (HALF, depth), 1)
    diagonal = own == lane % HALF
    outs = (left_ref, right_ref)
    for c in range(CHUNKS):
        copies[c].wait()
        for h in range(cols // HALF):
            summed = []
            for y in range(c * step, (c + 1) * step):
                row = jnp.broadcast_to(wide[h, pl.ds(y, 1), :], (HALF, depth))
                row = jnp.where(diagonal, row, 0.0)
                high = row.astype(BF16)
                low = (row - high.astype(F32)).astype(BF16)
                block = dev[:, y, h * HALF : (h + 1) * HALF, :].reshape(depth, runs)
                both = jnp.dot(
                    jnp.concatenate([high, low], axis=0), block, preferred_element_type=F32
                )
                summed.append(both[:HALF] + both[HALF:])
            group = jnp.concatenate(summed, axis=0).T.astype(BF16)
            per = CELLS // (step * HALF)
            width = step * HALF
            outs[h][c // per, :, (c % per) * width : (c % per + 1) * width] = group


def assemble_kernel(low_ref, left_ref, right_ref, high_ref, top_ref, bottom_ref):
    for i, ref in enumerate((low_ref, left_ref, right_ref, high_ref)):
        top_ref[i] = ref[0]
        bottom_ref[i] = ref[1]


def tables(place_ref, class_ref, codes_ref, col_bands, row_bands):
    shape = (HALF, place_ref.shape[1])
    u = jnp.broadcast_to(place_ref[0:1, :], shape).astype(F32).astype(BF16)
    v = place_ref[1:2, :]
    x = lax.broadcasted_iota(jnp.int32, shape, 0)
    side = HALF // 4 * (1 + class_ref[...])
    radius_sq = side * side
    column = {}
    for band in col_bands:
        gap = x + HALF * (band - 1) - v
        column[band] = (gap * gap).astype(F32).astype(BF16)
    reach = {}
    for band_row in row_bands:
        for band in col_bands:
            dr, ds = (band_row + 1) // 2, (band + 1) // 2
            if (dr, ds) in reach:
                continue
            code = 3 * dr + ds
            named = codes_ref[0:1, :] == code
            for e in range(1, 4):
                named = named | (codes_ref[e : e + 1, :] == code)
            kept = jnp.where(named, radius_sq, 0)
            reach[dr, ds] = jnp.broadcast_to(kept, shape).astype(F32).astype(BF16)
    return u, column, reach


def project(window, place_ref, class_ref, codes_ref, blocks):
    col_bands = sorted({b for _, b, _ in blocks})
    row_bands = sorted({a for a, _, _ in blocks})
    u, column, reach = tables(place_ref, class_ref, codes_ref, col_bands, row_bands)
    slots = place_ref.shape[1]
    wide = 256
    parts = []
    for n in range(slots // wide):
        cut = slice(n * wide, (n + 1) * wide)
        total = None
        for row_band in row_bands:
            squares = []
            for y in range(HALF):
                gap = jnp.asarray(y + HALF * (row_band - 1), BF16) - u[:, cut]
                squares.append(gap * gap)
            for a, b, source in blocks:
                if a != row_band:
                    continue
                limit = reach[(a + 1) // 2, (b + 1) // 2][:, cut]
                across = column[b][:, cut]
                pieces = []
                for y in range(HALF):
                    m = jnp.maximum((limit - squares[y]) - across, jnp.asarray(0, BF16))
                    pieces.append(m * m)
                taper = jnp.concatenate(pieces, axis=0)
                term = jnp.dot(window(source), taper, preferred_element_type=F32)
                total = term if total is None else total + term
        parts.append(total)
    return parts


def reduce_kernel(window, blocks, place_ref, class_ref, codes_ref, sensed_ref, out_ref):
    parts = project(window, place_ref, class_ref, codes_ref, blocks)
    for n, part in enumerate(parts):
        wide = part.shape[1]
        cut = slice(n * wide, (n + 1) * wide)
        out_ref[:, cut] = jnp.sum(part * sensed_ref[:, cut].astype(F32), axis=0, keepdims=True)


def inner_kernel(
    tally_hbm,
    left_ref,
    right_ref,
    place_ref,
    class_ref,
    codes_ref,
    sensed_ref,
    scaled_ref,
    out_ref,
    weight_ref,
    tally_ref,
    sem,
):
    copy = pltpu.make_async_copy(tally_hbm, tally_ref, sem)
    copy.start()
    blocks = [(1 + y, 1 + h, (h, y)) for h in range(2) for y in range(2)]
    refs = (left_ref, right_ref)
    reduce_kernel(
        lambda s: refs[s[0]][s[1]], blocks, place_ref, class_ref, codes_ref, sensed_ref, out_ref
    )
    side = (HALF // 4 * (1 + class_ref[...])).astype(F32)
    radius_sq = side * side
    weight = scaled_ref[...] / (radius_sq * radius_sq) / (sensed_ref.shape[0] - 1)
    slot = lax.broadcasted_iota(jnp.int32, weight.shape, 1)
    copy.wait()
    weight_ref[...] = jnp.where(slot < tally_ref[0, 0], weight, 0.0)


def sides_kernel(low_ref, high_ref, place_ref, class_ref, codes_ref, sensed_ref, out_ref):
    blocks = [(1 + y, 3 * h, (h, y)) for h in range(2) for y in range(2)]
    refs = (low_ref, high_ref)
    reduce_kernel(
        lambda s: refs[s[0]][s[1]], blocks, place_ref, class_ref, codes_ref, sensed_ref, out_ref
    )


def outer_kernel(
    above_ref,
    below_ref,
    place_ref,
    class_ref,
    codes_ref,
    sensed_ref,
    inner_ref,
    sides_ref,
    weight_ref,
    out_ref,
):
    blocks = [(3 * h, b, (h, b)) for h in range(2) for b in range(4)]
    refs = (above_ref, below_ref)
    parts = project(lambda s: refs[s[0]][s[1]], place_ref, class_ref, codes_ref, blocks)
    for n, part in enumerate(parts):
        wide = part.shape[1]
        cut = slice(n * wide, (n + 1) * wide)
        summed = jnp.sum(part * sensed_ref[:, cut].astype(F32), axis=0, keepdims=True)
        summed = summed + inner_ref[:, cut] + sides_ref[:, cut]
        out_ref[:, cut] = weight_ref[:, cut] * summed


def on_device(
    prediction_deviation,
    humid_energy_misfit,
    sensor_space_deviation,
    scaled_departure,
    datum_location,
    taper_category,
    datum_patch_codes,
    active_datum_tally,
):
    levels, rows, cols, runs = prediction_deviation.shape
    slots = sensor_space_deviation.shape[3]
    vmem = pl.BlockSpec(memory_space=pltpu.VMEM)
    anywhere = pl.BlockSpec(memory_space=pl.ANY)
    half = pltpu.VMEM((2, runs, CELLS), BF16)
    strip = pltpu.VMEM((4, runs, CELLS), BF16)
    line = pltpu.VMEM((1, slots), F32)

    def near(*arrays):
        return [pltpu.with_memory_space_constraint(a, pltpu.VMEM) for a in arrays]

    left, right = pl.pallas_call(
        level_sum_kernel,
        out_shape=(half, half),
        in_specs=[anywhere, anywhere],
        out_specs=(vmem, vmem),
        scratch_shapes=[
            pltpu.VMEM((levels, rows, cols, runs), BF16),
            pltpu.VMEM((levels, rows, cols), F32),
            pltpu.VMEM((2, rows, levels * HALF), F32),
            pltpu.SemaphoreType.DMA((CHUNKS + 1,)),
        ],
        name="level_sum",
    )(prediction_deviation, humid_energy_misfit)

    def shift(block, axis, by):
        count = lax.axis_size(axis)
        return lax.ppermute(block, axis, [(i, (i + by) % count) for i in range(count)])

    low = shift(right, "lon", 1)
    high = shift(left, "lon", -1)

    place = datum_location[0, 0]
    category = taper_category[0]
    codes = datum_patch_codes[0, 0]
    sensed = sensor_space_deviation[0, 0]

    def cost(blocks):
        flops = 2 * runs * blocks * CELLS * slots
        return pl.CostEstimate(flops=flops, transcendentals=0, bytes_accessed=runs * 4096)

    inner, weight = pl.pallas_call(
        inner_kernel,
        out_shape=(line, line),
        in_specs=[anywhere] + [vmem] * 7,
        out_specs=(vmem, vmem),
        scratch_shapes=[pltpu.SMEM((1, 1), jnp.int32), pltpu.SemaphoreType.DMA],
        cost_estimate=cost(4),
        name="inner",
    )(active_datum_tally, *near(left, right, place, category, codes, sensed, scaled_departure[0]))
    top, bottom = pl.pallas_call(
        assemble_kernel,
        out_shape=(strip, strip),
        in_specs=[vmem] * 4,
        out_specs=(vmem, vmem),
        name="assemble",
    )(*near(low, left, right, high))
    above = shift(bottom, "lat", 1)
    below = shift(top, "lat", -1)
    sides = pl.pallas_call(
        sides_kernel,
        out_shape=line,
        in_specs=[vmem] * 6,
        out_specs=vmem,
        cost_estimate=cost(4),
        name="sides",
    )(*near(low, high, place, category, codes, sensed))
    impact = pl.pallas_call(
        outer_kernel,
        out_shape=jax.ShapeDtypeStruct((1, slots), F32),
        in_specs=[vmem] * 9,
        out_specs=vmem,
        cost_estimate=cost(8),
        name="outer",
    )(*near(above, below, place, category, codes, sensed, inner, sides, weight))
    return impact[None]


def solution(mesh):
    return jax.shard_map(
        on_device,
        mesh=mesh,
        in_specs=(
            P(None, "lat", "lon", None),
            P(None, "lat", "lon"),
            P("lat", "lon", None, None),
            P("lat", "lon", None),
            P("lat", "lon", None, None),
            P("lat", "lon", None),
            P("lat", "lon", None, None),
            P("lat", "lon"),
        ),
        out_specs=P("lat", "lon", None),
        check_vma=False,
    )
```

```python
import functools

import jax
import jax.numpy as jnp
from jax import lax
from jax.experimental import pallas as pl
from jax.experimental.pallas import tpu as pltpu
from jax.sharding import PartitionSpec as P

HALF = 16
CELLS = HALF * HALF
CHUNKS = 4

F32 = jnp.float32
BF16 = jnp.bfloat16


def level_sum_kernel(dev_hbm, misfit_hbm, left_ref, right_ref, dev, misfit_ref, wide, sems):
    levels, rows, cols, runs = dev.shape
    step = rows // CHUNKS
    first = pltpu.make_async_copy(misfit_hbm, misfit_ref, sems.at[CHUNKS])
    first.start()
    copies = []
    for c in range(CHUNKS):
        part = pl.ds(c * step, step)
        copies.append(pltpu.make_async_copy(dev_hbm.at[:, part], dev.at[:, part], sems.at[c]))
        copies[-1].start()
    first.wait()
    for h in range(cols // HALF):
        wide[h] = jnp.concatenate(
            [misfit_ref[l][:, h * HALF : (h + 1) * HALF] for l in range(levels)], axis=1
        )
    depth = levels * HALF
    own = lax.broadcasted_iota(jnp.int32, (HALF, depth), 0)
    lane = lax.broadcasted_iota(jnp.int32, (HALF, depth), 1)
    diagonal = own == lane % HALF
    outs = (left_ref, right_ref)
    for c in range(CHUNKS):
        copies[c].wait()
        for h in range(cols // HALF):
            summed = []
            for y in range(c * step, (c + 1) * step):
                row = jnp.broadcast_to(wide[h, pl.ds(y, 1), :], (HALF, depth))
                row = jnp.where(diagonal, row, 0.0)
                high = row.astype(BF16)
                low = (row - high.astype(F32)).astype(BF16)
                block = dev[:, y, h * HALF : (h + 1) * HALF, :].reshape(depth, runs)
                both = jnp.dot(
                    jnp.concatenate([high, low], axis=0), block, preferred_element_type=F32
                )
                summed.append(both[:HALF] + both[HALF:])
            group = jnp.concatenate(summed, axis=0).T.astype(BF16)
            per = CELLS // (step * HALF)
            width = step * HALF
            outs[h][c // per, :, (c % per) * width : (c % per + 1) * width] = group


def assemble_kernel(low_ref, left_ref, right_ref, high_ref, after_ref, across_ref, within_ref):
    odd = lax.axis_index("lat") % 2
    for i, ref in enumerate((low_ref, left_ref, right_ref, high_ref)):
        across_ref[i] = ref[odd]
        within_ref[i] = ref[1 - odd]


def tables(place_ref, class_ref, codes_ref, col_bands, row_bands):
    shape = (HALF, place_ref.shape[1])
    x = lax.broadcasted_iota(jnp.int32, shape, 0)
    side = HALF // 4 * (1 + class_ref[...])
    radius_sq = side * side
    column = {}
    for band in col_bands:
        gap = x + HALF * (band - 1) - place_ref[1:2, :]
        column[band] = (gap * gap).astype(F32).astype(BF16)
    rows, reach = [], []
    for first, dr in row_bands:
        rows.append(jnp.broadcast_to(place_ref[0:1, :] - first, shape).astype(F32).astype(BF16))
        limits = {}
        for band in col_bands:
            ds = (band + 1) // 2
            if ds in limits:
                continue
            code = 3 * dr + ds
            named = codes_ref[0:1, :] == code
            for e in range(1, 4):
                named = named | (codes_ref[e : e + 1, :] == code)
            kept = jnp.where(named, radius_sq, 0)
            limits[ds] = jnp.broadcast_to(kept, shape).astype(F32).astype(BF16)
        reach.append(limits)
    return rows, column, reach


def project(place_ref, class_ref, codes_ref, row_bands, col_bands, window):
    rows, column, reach = tables(place_ref, class_ref, codes_ref, col_bands, row_bands)
    slots = place_ref.shape[1]
    wide = 256
    parts = []
    for n in range(slots // wide):
        cut = slice(n * wide, (n + 1) * wide)
        total = None
        for i in range(len(row_bands)):
            squares = []
            for y in range(HALF):
                gap = jnp.asarray(y, BF16) - rows[i][:, cut]
                squares.append(gap * gap)
            for j, band in enumerate(col_bands):
                limit = reach[i][(band + 1) // 2][:, cut]
                across = column[band][:, cut]
                pieces = []
                for y in range(HALF):
                    m = jnp.maximum((limit - squares[y]) - across, jnp.asarray(0, BF16))
                    pieces.append(m * m)
                taper = jnp.concatenate(pieces, axis=0)
                term = jnp.dot(window(i, j), taper, preferred_element_type=F32)
                total = term if total is None else total + term
        parts.append(total)
    return parts


OWN_ROWS = ((0, 1), (HALF, 1))


def reduce_kernel(first_ref, second_ref, place_ref, class_ref, codes_ref, sensed_ref, out_ref, cols):
    refs = (first_ref, second_ref)
    parts = project(
        place_ref, class_ref, codes_ref, OWN_ROWS, cols, lambda row, col: refs[col][row]
    )
    for n, part in enumerate(parts):
        wide = part.shape[1]
        cut = slice(n * wide, (n + 1) * wide)
        out_ref[:, cut] = jnp.sum(part * sensed_ref[:, cut].astype(F32), axis=0, keepdims=True)


def inner_kernel(
    tally_ref,
    left_ref,
    right_ref,
    place_ref,
    class_ref,
    codes_ref,
    sensed_ref,
    scaled_ref,
    out_ref,
    weight_ref,
):
    reduce_kernel(
        left_ref, right_ref, place_ref, class_ref, codes_ref, sensed_ref, out_ref, (1, 2)
    )
    side = (HALF // 4 * (1 + class_ref[...])).astype(F32)
    radius_sq = side * side
    weight = scaled_ref[...] / (radius_sq * radius_sq) / (sensed_ref.shape[0] - 1)
    slot = lax.broadcasted_iota(jnp.int32, weight.shape, 1)
    weight_ref[...] = jnp.where(slot < tally_ref[0, 0], weight, 0.0)


def sides_kernel(low_ref, high_ref, place_ref, class_ref, codes_ref, sensed_ref, out_ref):
    reduce_kernel(low_ref, high_ref, place_ref, class_ref, codes_ref, sensed_ref, out_ref, (0, 3))


def strip_kernel(across, strip_ref, place_ref, class_ref, codes_ref, sensed_ref, *refs):
    odd = lax.axis_index("lat") % 2
    below = odd if across else 1 - odd
    row_bands = ((3 * HALF * below - HALF, 2 * below),)
    parts = project(
        place_ref, class_ref, codes_ref, row_bands, (0, 1, 2, 3), lambda row, col: strip_ref[col]
    )
    *others, out_ref = refs
    for n, part in enumerate(parts):
        wide = part.shape[1]
        cut = slice(n * wide, (n + 1) * wide)
        summed = jnp.sum(part * sensed_ref[:, cut].astype(F32), axis=0, keepdims=True)
        if others:
            weight_ref, *sums = others
            for ref in sums:
                summed = summed + ref[:, cut]
            summed = weight_ref[:, cut] * summed
        out_ref[:, cut] = summed


def on_device(
    prediction_deviation,
    humid_energy_misfit,
    sensor_space_deviation,
    scaled_departure,
    datum_location,
    taper_category,
    datum_patch_codes,
    active_datum_tally,
):
    levels, rows, cols, runs = prediction_deviation.shape
    slots = sensor_space_deviation.shape[3]
    vmem = pl.BlockSpec(memory_space=pltpu.VMEM)
    anywhere = pl.BlockSpec(memory_space=pl.ANY)
    half = pltpu.VMEM((2, runs, CELLS), BF16)
    strip = pltpu.VMEM((4, runs, CELLS), BF16)
    line = pltpu.VMEM((1, slots), F32)

    def near(*arrays):
        return [pltpu.with_memory_space_constraint(a, pltpu.VMEM) for a in arrays]

    left, right = pl.pallas_call(
        level_sum_kernel,
        out_shape=(half, half),
        in_specs=[anywhere, anywhere],
        out_specs=(vmem, vmem),
        scratch_shapes=[
            pltpu.VMEM((levels, rows, cols, runs), BF16),
            pltpu.VMEM((levels, rows, cols), F32),
            pltpu.VMEM((2, rows, levels * HALF), F32),
            pltpu.SemaphoreType.DMA((CHUNKS + 1,)),
        ],
        name="level_sum",
    )(prediction_deviation, humid_energy_misfit)

    def shift(block, axis, by):
        count = lax.axis_size(axis)
        return lax.ppermute(block, axis, [(i, (i + by) % count) for i in range(count)])

    low = shift(right, "lon", 1)
    high = shift(left, "lon", -1)

    place = datum_location[0, 0]
    category = taper_category[0]
    codes = datum_patch_codes[0, 0]
    sensed = sensor_space_deviation[0, 0]

    def cost(blocks):
        flops = 2 * runs * blocks * CELLS * slots
        return pl.CostEstimate(flops=flops, transcendentals=0, bytes_accessed=runs * 4096)

    inner, weight = pl.pallas_call(
        inner_kernel,
        out_shape=(line, line),
        in_specs=[pl.BlockSpec(memory_space=pltpu.SMEM)] + [vmem] * 7,
        out_specs=(vmem, vmem),
        cost_estimate=cost(4),
        name="inner",
    )(active_datum_tally, *near(left, right, place, category, codes, sensed, scaled_departure[0]))
    across, within = pl.pallas_call(
        assemble_kernel,
        out_shape=(strip, strip),
        in_specs=[vmem] * 5,
        out_specs=(vmem, vmem),
        name="assemble",
    )(*near(low, left, right, high, inner))

    def swap(block, first):
        count = lax.axis_size("lat")
        lower = range(first, count - 1, 2)
        return lax.ppermute(
            block, "lat", [(i, i + 1) for i in lower] + [(i + 1, i) for i in lower]
        )

    across = swap(across, 1)
    within = swap(within, 0)
    sides = pl.pallas_call(
        sides_kernel,
        out_shape=line,
        in_specs=[vmem] * 6,
        out_specs=vmem,
        cost_estimate=cost(4),
        name="sides",
    )(*near(low, high, place, category, codes, sensed))
    within = pl.pallas_call(
        functools.partial(strip_kernel, False),
        out_shape=line,
        in_specs=[vmem] * 5,
        out_specs=vmem,
        cost_estimate=cost(4),
        name="within_strip",
    )(*near(within, place, category, codes, sensed))
    impact = pl.pallas_call(
        functools.partial(strip_kernel, True),
        out_shape=jax.ShapeDtypeStruct((1, slots), F32),
        in_specs=[vmem] * 9,
        out_specs=vmem,
        cost_estimate=cost(4),
        name="across_strip",
    )(*near(across, place, category, codes, sensed, weight, inner, sides, within))
    return impact[None]


def solution(mesh):
    return jax.shard_map(
        on_device,
        mesh=mesh,
        in_specs=(
            P(None, "lat", "lon", None),
            P(None, "lat", "lon"),
            P("lat", "lon", None, None),
            P("lat", "lon", None),
            P("lat", "lon", None, None),
            P("lat", "lon", None),
            P("lat", "lon", None, None),
            P("lat", "lon"),
        ),
        out_specs=P("lat", "lon", None),
        check_vma=False,
    )
```
